512 devices in a mesh: grp: 8 (over x, core), wide: 64 (over y, z).
Axes of the slice: x: 4, y: 4, z: 16, core: 2. Of those that a mesh axis runs over, the one named last changes fastest.
Arguments:
- cluster_coefficients: bfloat16 [512, 24576], P(('grp', 'wide')), may hold values from -6 to 6
- exchange_repulsion_matrix: bfloat16 [512, 24576], P(('grp', 'wide')), may hold values from -6 to 6
- quadruple_virtual_tensor: bfloat16 [24576, 24576], P('grp', 'wide'), may hold values from -0.0546875 to 0.0546875
- retained_submatrix_flags: int32 [384, 384], P('grp', 'wide'), may hold values 0 or 1
- front_group_coupling_matrix: float32 [6, 64, 64], replicated, may hold values from -0.6 to 0.6
- rear_group_coupling_matrix: float32 [6, 64, 64], replicated, may hold values from -0.6 to 0.6
- hole_level_sums: float32 [512], P(('grp', 'wide')), may hold values from -2 to -0.5
- particle_level_sums: float32 [24576], replicated, may hold values from 0.5 to 4
Outputs:
- increment: float32 [512, 24576], P(('grp', 'wide'))
The draws below stay inside these ranges and needn't reach their ends.
All inputs are finite; a program needn't handle non-finite values. No bound on the sum of `retained_submatrix_flags` on one device may be relied on, other than what follows from the above.
Results may differ from the reference program's by a relative error of at most 0.0003.
Values may be sent and summed in bfloat16 or wider, within the bound.
A program may use at most 64 MiB of HBM per device.

```python
import jax
import jax.numpy as jnp
from jax import lax

GROUP_WIDTH = 64
NTP = 6
WINDOW_VIRTPAIRS = 24576
PAIR_COUNT = 512


def with_ends(result, rng, least, high):
    place = [jax.random.randint(jax.random.fold_in(rng, axis), (), 0, length) for axis, length in enumerate(result.shape)]
    longest = result.shape.index(max(result.shape))
    next_to = place[:longest] + [(place[longest] + 1) % result.shape[longest]] + place[longest + 1:]
    return result.at[tuple(place)].set(least).at[tuple(next_to)].set(high)


def levels(key, dims, cuts, least, largest):
    level, own = 1.0, jax.random.fold_in(key, 6)
    for dim, shards_of in cuts:
        steps = jnp.exp(jax.random.uniform(jax.random.fold_in(own, dim), (shards_of,), jnp.float32, least / len(cuts), largest / len(cuts)))
        level = level * jnp.repeat(steps, dims[dim] // shards_of).reshape([-1 if axis == dim else 1 for axis in range(len(dims))])
    return level


def noise(rng, extent, deviation, reach, shards=(), held_as=jnp.bfloat16):
    loudness = levels(rng, extent, shards, -0.22, 0.18) if shards else 1.0
    result = jax.random.normal(rng, extent, jnp.float32) * deviation * loudness
    return jnp.minimum(jnp.maximum(result, -reach), reach).astype(held_as)


def setup_inputs(seed: int = 0) -> dict:
    key_of = jax.random.split(jax.random.key(seed), 9)
    return {
        "cluster_coefficients": noise(key_of[0], (PAIR_COUNT, WINDOW_VIRTPAIRS), 1.0, 6.0, ((0, 512),)),
        "exchange_repulsion_matrix": noise(key_of[1], (PAIR_COUNT, WINDOW_VIRTPAIRS), 1.0, 6.0, ((0, 512),)),
        "quadruple_virtual_tensor": noise(key_of[2], (WINDOW_VIRTPAIRS, WINDOW_VIRTPAIRS), (WINDOW_VIRTPAIRS // 2) ** -0.5, 0.0546875, ((0, 8), (1, 64))),
        "retained_submatrix_flags": with_ends((jax.random.randint(key_of[3], (WINDOW_VIRTPAIRS // GROUP_WIDTH, WINDOW_VIRTPAIRS // GROUP_WIDTH), 0, 2) < 1).astype(jnp.int32), jax.random.fold_in(key_of[3], 1), 0, 1),
        "front_group_coupling_matrix": noise(key_of[4], (NTP, GROUP_WIDTH, GROUP_WIDTH), 0.1, 0.6, (), jnp.float32),
        "rear_group_coupling_matrix": noise(key_of[5], (NTP, GROUP_WIDTH, GROUP_WIDTH), 0.1, 0.6, (), jnp.float32),
        "hole_level_sums": jnp.clip(-2.0 + 1.5 * jax.random.uniform(key_of[6], (PAIR_COUNT,), jnp.float32) ** levels(key_of[6], (PAIR_COUNT,), ((0, 512),), -0.2, 0.2), -2.0, -0.5),
        "particle_level_sums": jnp.clip(jax.random.uniform(key_of[7], (WINDOW_VIRTPAIRS,), jnp.float32, 0.5, 4.0), 0.5, 4.0),
    }


def reference(cluster_coefficients, exchange_repulsion_matrix, quadruple_virtual_tensor, retained_submatrix_flags, front_group_coupling_matrix, rear_group_coupling_matrix, hole_level_sums, particle_level_sums):
    blocks = WINDOW_VIRTPAIRS // GROUP_WIDTH
    kept_column_flags = jnp.repeat(retained_submatrix_flags, GROUP_WIDTH, axis=1).astype(jnp.bfloat16)
    pruned_particle_contraction = (quadruple_virtual_tensor.reshape(blocks, GROUP_WIDTH, WINDOW_VIRTPAIRS) * kept_column_flags[:, None, :]).reshape(WINDOW_VIRTPAIRS, WINDOW_VIRTPAIRS)
    ladder = jnp.dot(cluster_coefficients, pruned_particle_contraction, preferred_element_type=jnp.float32)
    local_amplitude_block = cluster_coefficients.astype(jnp.float32).reshape(PAIR_COUNT, NTP, GROUP_WIDTH, GROUP_WIDTH)
    leading_term = jnp.einsum("khd,jkdw->jkhw", front_group_coupling_matrix.astype(jnp.float32), local_amplitude_block, precision=lax.Precision.HIGHEST)
    second_term = jnp.einsum("tbd,ptad->ptab", rear_group_coupling_matrix.astype(jnp.float32), local_amplitude_block, precision=lax.Precision.HIGHEST)
    fock_term = (leading_term + second_term).reshape(PAIR_COUNT, WINDOW_VIRTPAIRS)
    residual = exchange_repulsion_matrix.astype(jnp.float32) + fock_term + ladder
    return residual / (particle_level_sums[None, :] - hole_level_sums[:, None])
```

```python
import jax
import jax.numpy as jnp
from jax import lax
from jax.experimental import pallas as pl
from jax.experimental.pallas import tpu as pltpu
from jax.sharding import PartitionSpec as P

MESH = pl.DeviceIdType.MESH
F32 = jnp.float32
BF16 = jnp.bfloat16

NG = 8
NY = 4
NZ = 16
NW = 64
KG = 3072
KH = 1536
KA = 512
KB = 1024
Q = 384
NQ = 192


def kernel(
    t_hbm, e_hbm, v_hbm, fl_hbm, f_hbm, r_hbm, hls, pls_hbm,
    out,
    trow, erow, vbuf, fl, mask, fbuf, rbuf, pls, tnat, base, inv,
    asrc, arecv, ta, tb, obuf, sbuf, xr, fs, lad,
    ld_sem, a_send, a_recv, ay_recv, az_recv, bz_recv, by_recv, x_recv, l_recv,
    ta_send, tb_send, x_send, l_send,
):
    g = lax.axis_index("grp")
    w = lax.axis_index("wide")
    y = w // NZ
    z = w % NZ

    def wid(yy, zz):
        return lax.rem(yy + 2 * NY, NY) * NZ + lax.rem(zz + 2 * NZ, NZ)

    def rcopy(src, dst, ss, rs, gg, ww):
        return pltpu.make_async_remote_copy(
            src_ref=src, dst_ref=dst, send_sem=ss, recv_sem=rs,
            device_id=(gg, ww), device_id_type=MESH,
        )

    loads = [
        pltpu.make_async_copy(s, d, ld_sem.at[i])
        for i, (s, d) in enumerate([
            (t_hbm, trow), (fl_hbm, fl), (v_hbm, vbuf), (f_hbm, fbuf),
            (r_hbm, rbuf), (e_hbm, erow), (pls_hbm, pls),
        ])
    ]
    for c in loads:
        c.start()

    barrier = pltpu.get_barrier_semaphore()
    for d in range(1, NG):
        pl.semaphore_signal(barrier, inc=1, device_id=(lax.rem(g + d, NG), w), device_id_type=MESH)
    for ww in (wid(y + 1, z), wid(y - 1, z), wid(y + 2, z), wid(y, z + 1), wid(y, z - 1)):
        pl.semaphore_signal(barrier, inc=1, device_id=(g, ww), device_id_type=MESH)

    loads[0].wait()
    row = trow[...].astype(F32)
    for d in range(NG):
        asrc[d] = row[:, d * KG:(d + 1) * KG]
    pl.semaphore_wait(barrier, NG - 1 + 5)

    for d in range(1, NG):
        gg = lax.rem(g + d, NG)
        rcopy(asrc.at[gg], arecv.at[g], a_send, a_recv, gg, w).start()
    arecv[g] = asrc[g]

    loads[1].wait()
    qi = lax.broadcasted_iota(jnp.int32, (6, Q), 1) // 64
    onehot = jnp.where(qi == lax.broadcasted_iota(jnp.int32, (6, Q), 0), 1.0, 0.0).astype(F32)
    mask[...] = lax.dot_general(
        fl[...].astype(F32), onehot, (((0,), (0,)), ((), ())), preferred_element_type=F32
    )
    rcopy(asrc.at[pl.ds(0, NG - 1)], arecv.at[pl.ds(0, NG - 1)], a_send, a_recv, g, w).wait_recv()

    for gg in range(NG):
        tnat[pl.ds(gg, 1), :] = arecv[gg]
    lo, hi = tnat[:, :KH], tnat[:, KH:]
    ta[w] = jnp.concatenate([lo[:, :KA], hi[:, :KA]], axis=0).astype(BF16)
    tb[w] = jnp.concatenate([lo[:, KA:], hi[:, KA:]], axis=0).astype(BF16)

    zp, zm = wid(y, z + 1), wid(y, z - 1)
    yp, ym, y2 = wid(y + 1, z), wid(y - 1, z), wid(y + 2, z)
    zn = (zp, zm)

    def send_a(blk, ww, rs):
        rcopy(ta.at[blk], ta.at[blk], ta_send, rs, g, ww).start()

    def send_b(blk, ww, rs):
        rcopy(tb.at[blk], tb.at[blk], tb_send, rs, g, ww).start()

    def wait_a(blk, rs):
        rcopy(ta.at[blk], ta.at[blk], ta_send, rs, g, w).wait_recv()

    def wait_b(blk, rs):
        rcopy(tb.at[blk], tb.at[blk], tb_send, rs, g, w).wait_recv()

    send_a(w, yp, ay_recv.at[0])
    send_a(w, ym, ay_recv.at[1])
    send_a(w, y2, ay_recv.at[2])
    for d in range(2):
        send_b(w, zn[d], bz_recv.at[d, 1])
        send_a(w, zn[d], az_recv.at[d, 1, 0])
    send_b(w, yp, by_recv.at[0, 1, 0])
    send_b(w, ym, by_recv.at[0, 1, 1])

    loads[2].wait()

    def screen(i, _):
        m = mask[pl.ds(i, 1), :].astype(BF16)
        rows = pl.ds(pl.multiple_of(i * 64, 64), 64)
        vbuf[rows, :] = vbuf[rows, :] * m
        return 0

    lax.fori_loop(0, 48, screen, 0)

    for slot, dy in ((0, 3), (1, 1), (2, 2)):
        blk = wid(y + dy, z)
        wait_a(blk, ay_recv.at[slot])
        for d in range(2):
            send_a(blk, zn[d], az_recv.at[d, 1, dy])

    for c in loads[3:]:
        c.wait()

    def fock(t, _):
        rows = pl.ds(pl.multiple_of(t * 32, 32), 32)
        for k in range(32):
            o = pl.multiple_of(t * 4096 + k * 128, 128)
            base[pl.ds(t * 32 + k, 1), :] = trow[:, pl.ds(o, 128)].astype(F32)
        x = base[rows, :]
        xr_ = jnp.concatenate([x[:, :64], x[:, 64:]], axis=0).astype(BF16)
        i0 = lax.broadcasted_iota(jnp.int32, (64, 64), 0)
        i1 = lax.broadcasted_iota(jnp.int32, (64, 64), 1)
        perm = jnp.where(i1 == lax.rem(i0, 32) * 2 + i0 // 32, 1.0, 0.0).astype(BF16)
        dn = (((1,), (0,)), ((), ()))
        dt = (((1,), (1,)), ((), ()))
        dl = (((0,), (0,)), ((), ()))
        f = fbuf[t]
        fh = f.astype(BF16)
        fl_ = (f - fh.astype(F32)).astype(BF16)
        r = rbuf[t]
        rh = r.astype(BF16)
        rl = (r - rh.astype(F32)).astype(BF16)
        dot = lambda a, b, d: lax.dot_general(a, b, d, preferred_element_type=F32)
        c = dot(perm, xr_, dl).astype(BF16)
        fph = dot(perm, fh, dn).astype(BF16)
        fpl = dot(perm, fl_, dn).astype(BF16)
        o = dot(fph, c, dn) + dot(fpl, c, dn) + dot(xr_, rh, dt) + dot(xr_, rl, dt)
        base[rows, :] = jnp.concatenate([o[:32], o[32:]], axis=1)
        return 0

    lax.fori_loop(0, 6, fock, 0)

    h = hls[0]

    def finish_base(k, _):
        o = pl.multiple_of(k * 128, 128)
        lad_b = base[pl.ds(k, 1), :] + erow[:, pl.ds(o, 128)].astype(F32)
        inv[k] = 1.0 / (pls[k] - h)
        base[pl.ds(k, 1), :] = lad_b
        return 0

    lax.fori_loop(0, NQ, finish_base, 0)

    def col(s, d):
        return z - s if d == 0 else z + lax.rem(s, 8)

    def step(i, _):
        @pl.when(i <= 8)
        def _():
            for d in range(2):
                last = 8 - d

                @pl.when(i <= last)
                def _():
                    cz = col(i, d)
                    blk = wid(y, cz)
                    wait_b(blk, bz_recv.at[d, i])

                    @pl.when(i < last)
                    def _():
                        send_b(blk, zn[d], bz_recv.at[d, i + 1])

                    send_b(blk, yp, by_recv.at[i, d, 0])
                    send_b(blk, ym, by_recv.at[i, d, 1])
            for dy in (0, 3, 1, 2):
                for d in range(2):
                    last = 8 - d

                    @pl.when(i <= last)
                    def _():
                        blk = wid(y + dy, col(i, d))
                        wait_a(blk, az_recv.at[d, i, dy])

                        @pl.when(i < last)
                        def _():
                            send_a(blk, zn[d], az_recv.at[d, i + 1, dy])

        s1 = i - 1

        @pl.when((s1 >= 1) & (s1 <= 8))
        def _():
            blk = wid(y - 1, col(s1, 0))
            wait_b(blk, by_recv.at[s1, 0, 0])
            send_b(blk, yp, by_recv.at[s1, 0, 2])

        @pl.when(s1 <= 7)
        def _():
            blk = wid(y + 1, col(s1, 1))
            wait_b(blk, by_recv.at[s1, 1, 1])
            send_b(blk, ym, by_recv.at[s1, 1, 2])

        s2 = i - 2

        @pl.when((s2 >= 1) & (s2 <= 8))
        def _():
            s = s2
            sm = lax.rem(s, 8)
            wait_b(wid(y + 1, col(s, 0)), by_recv.at[s, 0, 1])
            wait_b(wid(y + 2, col(s, 0)), by_recv.at[s, 0, 2])
            wait_b(wid(y - 1, col(s, 1)), by_recv.at[sm, 1, 0])
            wait_b(wid(y + 2, col(s, 1)), by_recv.at[sm, 1, 2])
            blks = [wid(y + dy, col(s, d)) for d in range(2) for dy in range(NY)]
            xa = jnp.concatenate([ta[b] for b in blks], axis=0)
            xb = jnp.concatenate([tb[b] for b in blks], axis=0)
            total = None
            for hh in range(2):
                k0 = hh * KH
                o = jnp.dot(xa, vbuf[k0:k0 + KA, :], preferred_element_type=F32)
                o += jnp.dot(xb, vbuf[k0 + KA:k0 + KH, :], preferred_element_type=F32)
                o = o.reshape(8, 16, Q)[:, 8 * hh:8 * hh + 8, :]
                total = o if total is None else total + o
            total = total.reshape(64, Q)
            for c in range(3):
                obuf[c] = total[:, c * 128:(c + 1) * 128]
            for d in range(NG):
                for c in range(3):
                    sbuf[(s - 1) * NG + d, :, c * 128:(c + 1) * 128] = obuf[c, pl.ds(d, 8, stride=8), :]
            for d in range(1, NG):
                gg = lax.rem(g + d, NG)
                rcopy(sbuf.at[(s - 1) * NG + gg], xr.at[(s - 1) * NG + g], x_send, x_recv.at[s - 1], gg, w).start()
            xr[(s - 1) * NG + g] = sbuf[(s - 1) * NG + g]

        s3 = i - 3

        @pl.when((s3 >= 1) & (s3 <= 8))
        def _():
            s = s3
            win = pl.ds((s - 1) * NG, NG - 1)
            rcopy(sbuf.at[win], xr.at[win], x_send, x_recv.at[s - 1], g, w).wait_recv()
            tot = jnp.sum(xr[pl.ds((s - 1) * NG, NG)], axis=0)
            for n in range(8):
                for c in range(3):
                    fs[(s - 1) * 24 + 3 * n + c] = tot[n:n + 1, c * 128:(c + 1) * 128]
            for d in range(2):
                for dy in range(NY):
                    n = d * NY + dy
                    src = fs.at[pl.ds((s - 1) * 24 + 3 * n, 3)]

                    def push():
                        rcopy(src, lad.at[pl.ds(3 * w, 3)], l_send, l_recv, g, wid(y + dy, col(s, d))).start()

                    if d == 1 and dy == 0:
                        pl.when(s < 8)(push)

                        @pl.when(s == 8)
                        def _():
                            for c in range(3):
                                lad[3 * w + c] = fs[(s - 1) * 24 + 3 * n + c]
                    else:
                        push()
        return 0

    lax.fori_loop(1, 12, step, 0)

    part = pl.ds(0, 3 * (NW - 1))
    rcopy(fs.at[part], lad.at[part], l_send, l_recv, g, w).wait_recv()

    def finish(k, _):
        out[k] = (lad[k] + base[pl.ds(k, 1), :]) * inv[k]
        return 0

    lax.fori_loop(0, NQ, finish, 0)

    rcopy(asrc.at[pl.ds(0, NG - 1)], arecv.at[pl.ds(0, NG - 1)], a_send, a_recv, g, w).wait_send()
    rcopy(ta.at[pl.ds(0, NW - 1)], ta.at[pl.ds(0, NW - 1)], ta_send, ay_recv.at[0], g, w).wait_send()
    rcopy(tb.at[pl.ds(0, NW - 1)], tb.at[pl.ds(0, NW - 1)], tb_send, ay_recv.at[0], g, w).wait_send()
    rcopy(sbuf.at[pl.ds(0, 56)], xr.at[pl.ds(0, 56)], x_send, x_recv.at[0], g, w).wait_send()
    rcopy(fs.at[part], lad.at[part], l_send, l_recv, g, w).wait_send()


def local(t, e, v, flags, f, r, hls, pls):
    any_spec = pl.BlockSpec(memory_space=pl.ANY)
    vm = pltpu.VMEM
    dma = pltpu.SemaphoreType.DMA
    res = pl.pallas_call(
        kernel,
        out_shape=jax.ShapeDtypeStruct((NQ, 1, 128), F32),
        in_specs=[any_spec] * 6 + [pl.BlockSpec(memory_space=pltpu.SMEM), any_spec],
        out_specs=pl.BlockSpec(memory_space=pltpu.VMEM),
        scratch_shapes=[
            vm((1, 24576), BF16),
            vm((1, 24576), BF16),
            vm((KG, Q), BF16),
            vm((6, 48), jnp.int32),
            vm((48, Q), F32),
            vm((6, 64, 64), F32),
            vm((6, 64, 64), F32),
            vm((NQ, 1, 128), F32),
            vm((NG, KG), F32),
            vm((NQ, 128), F32),
            vm((NQ, 1, 128), F32),
            vm((NG, 1, KG), F32),
            vm((NG, 1, KG), F32),
            vm((NW, 16, KA), BF16),
            vm((NW, 16, KB), BF16),
            vm((3, 64, 128), F32),
            vm((64, 8, Q), F32),
            vm((64, 8, Q), F32),
            vm((NQ, 1, 128), F32),
            vm((NQ, 1, 128), F32),
            dma((7,)),
            dma,
            dma,
            dma((3,)),
            dma((2, 9, 4)),
            dma((2, 9)),
            dma((9, 2, 3)),
            dma((8,)),
            dma,
            dma,
            dma,
            dma,
            dma,
        ],
        compiler_params=pltpu.CompilerParams(
            collective_id=0, has_side_effects=True, vmem_limit_bytes=60 * 1024 * 1024
        ),
        name="ladder",
    )(t, e, v, flags.T, f, r, hls, pls.reshape(NQ, 1, 128))
    return res.reshape(1, 24576)


def solution(mesh):
    return jax.shard_map(
        local,
        mesh=mesh,
        in_specs=(
            P(("grp", "wide"), None),
            P(("grp", "wide"), None),
            P("grp", "wide"),
            P("grp", "wide"),
            P(),
            P(),
            P(("grp", "wide")),
            P(),
        ),
        out_specs=P(("grp", "wide"), None),
        check_vma=False,
    )
```

```python
import jax
import jax.numpy as jnp
from jax import lax
from jax.experimental import pallas as pl
from jax.experimental.pallas import tpu as pltpu
from jax.sharding import PartitionSpec as P

MESH = pl.DeviceIdType.MESH
F32 = jnp.float32
BF16 = jnp.bfloat16

NG = 8
NY = 4
NZ = 16
NW = 64
KG = 3072
KA = 512
KB = 1024
Q = 384
NQ = 192


def kernel(
    t_hbm, e_hbm, v_hbm, fl_hbm, f_hbm, r_hbm, hls, pls_hbm,
    out,
    trow, erow, vbuf, fl, mask, fbuf, rbuf, pls, tnat, base, base3, inv3,
    tsend, st0, stz, sty, scr, ta, tb, acc, obuf, sbuf, xr, fs, lad,
    ld_sem, s0_recv, sz_recv, sy_recv, az_recv, bz_recv, by_recv, x_recv, l_recv,
    s0_send, sz_send, sy_send, ta_send, tb_send, x_send, l_send,
):
    g = lax.axis_index("grp")
    w = lax.axis_index("wide")
    y = w // NZ
    z = w % NZ

    def wid(yy, zz):
        return lax.rem(yy + 2 * NY, NY) * NZ + lax.rem(zz + 2 * NZ, NZ)

    def rcopy(src, dst, ss, rs, gg, ww):
        return pltpu.make_async_remote_copy(
            src_ref=src, dst_ref=dst, send_sem=ss, recv_sem=rs,
            device_id=(gg, ww), device_id_type=MESH,
        )

    zp, zm = wid(y, z + 1), wid(y, z - 1)
    yp, ym, y2 = wid(y + 1, z), wid(y - 1, z), wid(y + 2, z)
    zn = (zp, zm)

    loads = [
        pltpu.make_async_copy(s, d, ld_sem.at[i])
        for i, (s, d) in enumerate([
            (t_hbm, trow), (fl_hbm, fl), (v_hbm, vbuf), (f_hbm, fbuf),
            (r_hbm, rbuf), (e_hbm, erow), (pls_hbm, pls),
        ])
    ]
    for c in loads:
        c.start()

    barrier = pltpu.get_barrier_semaphore()
    for d in range(NG):
        gg = lax.rem(g + d, NG)
        for ww in ((w,) if d else ()) + (zp, zm, yp, ym, y2):
            pl.semaphore_signal(barrier, inc=1, device_id=(gg, ww), device_id_type=MESH)

    loads[0].wait()
    for k in range(NQ):
        tnat[k:k + 1, :] = trow[:, k * 128:(k + 1) * 128].astype(F32)
    tsend[...] = tnat[...].astype(BF16).reshape(NG, 24, 128)
    pl.semaphore_wait(barrier, 6 * NG - 1)

    for d in range(NG):
        gg = lax.rem(g + d, NG)
        piece = tsend.at[gg]
        if d:
            rcopy(piece, st0.at[g], s0_send, s0_recv, gg, w).start()
        for slot, ww in ((0, yp), (1, ym), (2, y2)):
            rcopy(tsend.at[gg, pl.ds(0, 8)], sty.at[slot, g], sy_send, sy_recv.at[slot], gg, ww).start()
        for slot, ww in ((0, zp), (1, zm)):
            rcopy(tsend.at[gg, pl.ds(8, 16)], stz.at[slot, g], sz_send, sz_recv.at[slot], gg, ww).start()
    st0[g] = tsend[g]

    loads[1].wait()
    qi = lax.broadcasted_iota(jnp.int32, (6, Q), 1) // 64
    onehot = jnp.where(qi == lax.broadcasted_iota(jnp.int32, (6, Q), 0), 1.0, 0.0).astype(F32)
    mask[...] = lax.dot_general(
        fl[...].astype(F32), onehot, (((0,), (0,)), ((), ())), preferred_element_type=F32
    )
    loads[2].wait()

    def screen(i, _):
        m = mask[pl.ds(i, 1), :].astype(BF16)
        rows = pl.ds(pl.multiple_of(i * 64, 64), 64)
        vbuf[rows, :] = vbuf[rows, :] * m
        return 0

    lax.fori_loop(0, 48, screen, 0)

    for c in loads[3:]:
        c.wait()
    i0 = lax.broadcasted_iota(jnp.int32, (64, 64), 0)
    i1 = lax.broadcasted_iota(jnp.int32, (64, 64), 1)
    perm = jnp.where(i1 == lax.rem(i0, 32) * 2 + i0 // 32, 1.0, 0.0).astype(BF16)
    dn = (((1,), (0,)), ((), ()))
    dt = (((1,), (1,)), ((), ()))
    dl = (((0,), (0,)), ((), ()))

    def dot(a, b, d):
        return lax.dot_general(a, b, d, preferred_element_type=F32)

    for t in range(6):
        x = tnat[t * 32:(t + 1) * 32, :]
        xc = jnp.concatenate([x[:, :64], x[:, 64:]], axis=0).astype(BF16)
        f = fbuf[t]
        fh = f.astype(BF16)
        fl_ = (f - fh.astype(F32)).astype(BF16)
        r = rbuf[t]
        rh = r.astype(BF16)
        rl = (r - rh.astype(F32)).astype(BF16)
        c = dot(perm, xc, dl).astype(BF16)
        fph = dot(perm, fh, dn).astype(BF16)
        fpl = dot(perm, fl_, dn).astype(BF16)
        o = dot(fph, c, dn) + dot(fpl, c, dn) + dot(xc, rh, dt) + dot(xc, rl, dt)
        base[t * 32:(t + 1) * 32, :] = jnp.concatenate([o[:32], o[32:]], axis=1)

    inv3[...] = 1.0 / (pls[...] - hls[0])

    def add_exchange(k, _):
        for j in range(8):
            q = k * 8 + j
            o = pl.multiple_of(q * 128, 128)
            base3[q] = base[pl.ds(q, 1), :] + erow[:, pl.ds(o, 128)].astype(F32)
        return 0

    lax.fori_loop(0, NQ // 8, add_exchange, 0)

    def send_a(blk, ww, rs):
        rcopy(ta.at[blk], ta.at[blk], ta_send, rs, g, ww).start()

    def send_b(blk, ww, rs):
        rcopy(tb.at[blk], tb.at[blk], tb_send, rs, g, ww).start()

    def wait_a(blk, rs):
        rcopy(ta.at[blk], ta.at[blk], ta_send, rs, g, w).wait_recv()

    def wait_b(blk, rs):
        rcopy(tb.at[blk], tb.at[blk], tb_send, rs, g, w).wait_recv()

    def pack(staged, n, first, groups, dst, blk):
        scr[0:8 * n, :] = staged.astype(F32).reshape(8 * n, 128)
        for m in range(groups):
            top = scr[pl.ds(first + m, 8, stride=n), :]
            bottom = scr[pl.ds(first + groups + m, 8, stride=n), :]
            dst[blk, :, m * 128:(m + 1) * 128] = jnp.concatenate([top, bottom], axis=0).astype(BF16)

    def col(s, d):
        return z - s if d == 0 else z + s % 8

    rcopy(st0.at[pl.ds(0, 7)], st0.at[pl.ds(0, 7)], s0_send, s0_recv, g, w).wait_recv()
    pack(st0[...], 24, 0, 4, ta, w)
    for d in range(2):
        send_a(w, zn[d], az_recv.at[d, 1, 0])
    pack(st0[...], 24, 8, 8, tb, w)
    send_b(w, yp, by_recv.at[0, 1, 0])
    send_b(w, ym, by_recv.at[0, 1, 1])
    for d in range(2):
        rcopy(stz.at[d], stz.at[d], sz_send, sz_recv.at[d], g, w).wait_recv()
        blk = wid(y, col(1, d))
        pack(stz[d], 16, 0, 8, tb, blk)
        send_b(blk, zn[d], bz_recv.at[d, 2])
        send_b(blk, yp, by_recv.at[1, d, 0])
        send_b(blk, ym, by_recv.at[1, d, 1])
    for slot, dy in ((0, 3), (1, 1), (2, 2)):
        rcopy(sty.at[slot], sty.at[slot], sy_send, sy_recv.at[slot], g, w).wait_recv()
        blk = wid(y + dy, z)
        pack(sty[slot], 8, 0, 4, ta, blk)
        for d in range(2):
            send_a(blk, zn[d], az_recv.at[d, 1, dy])


    def z_b(s):
        for d in range(2):
            last = 8 - d
            if s > last:
                continue
            blk = wid(y, col(s, d))
            wait_b(blk, bz_recv.at[d, s])
            if s < last:
                send_b(blk, zn[d], bz_recv.at[d, s + 1])
            send_b(blk, yp, by_recv.at[s, d, 0])
            send_b(blk, ym, by_recv.at[s, d, 1])
            if s == 8:
                send_b(blk, y2, by_recv.at[s, d, 2])

    def z_a(s, dy):
        for d in range(2):
            last = 8 - d
            if s > last:
                continue
            blk = wid(y + dy, col(s, d))
            wait_a(blk, az_recv.at[d, s, dy])
            if s < last:
                send_a(blk, zn[d], az_recv.at[d, s + 1, dy])

    def y_b(s):
        if 1 <= s <= 7:
            blk = wid(y - 1, col(s, 0))
            wait_b(blk, by_recv.at[s, 0, 0])
            send_b(blk, yp, by_recv.at[s, 0, 2])
        if 0 <= s <= 7:
            blk = wid(y + 1, col(s, 1))
            wait_b(blk, by_recv.at[s, 1, 1])
            send_b(blk, ym, by_recv.at[s, 1, 2])

    def blocks(s):
        return [wid(y + dy, col(s, d)) for d in range(2) for dy in range(NY)]

    def half(o, h):
        return o.reshape(8, 16, Q)[:, 8 * h:8 * h + 8, :].reshape(64, Q)

    def comp_a(s):
        x = jnp.concatenate([ta[b] for b in blocks(s)], axis=0)
        o0 = jnp.dot(x, vbuf[0:KA, :], preferred_element_type=F32)
        o1 = jnp.dot(x, vbuf[KA:2 * KA, :], preferred_element_type=F32)
        acc[...] = half(o0, 0) + half(o1, 1)

    def comp_b(s, h):
        if h == 0:
            if s == 8:
                wait_b(wid(y - 1, col(s, 0)), by_recv.at[s, 0, 0])
            wait_b(wid(y + 1, col(s, 0)), by_recv.at[s, 0, 1])
            wait_b(wid(y + 2, col(s, 0)), by_recv.at[s, 0, 2])
            wait_b(wid(y - 1, col(s, 1)), by_recv.at[s % 8, 1, 0])
            wait_b(wid(y + 2, col(s, 1)), by_recv.at[s % 8, 1, 2])
        x = jnp.concatenate([tb[b] for b in blocks(s)], axis=0)
        k0 = 2 * KA + h * KB
        o = half(jnp.dot(x, vbuf[k0:k0 + KB, :], preferred_element_type=F32), h) + acc[...]
        if h == 0:
            acc[...] = o
            return
        for c in range(3):
            obuf[c] = o[:, c * 128:(c + 1) * 128]
        j = (s - 1) * NG
        for d in range(NG):
            for c in range(3):
                sbuf[j + d, :, c * 128:(c + 1) * 128] = obuf[c, pl.ds(d, 8, stride=8), :]
        for d in range(1, NG):
            gg = lax.rem(g + d, NG)
            rcopy(sbuf.at[j + gg], xr.at[j + g], x_send, x_recv.at[s - 1], gg, w).start()
        xr[j + g] = sbuf[j + g]

    def reduce(s):
        j = (s - 1) * NG
        win = pl.ds(j, NG - 1)
        rcopy(sbuf.at[win], xr.at[win], x_send, x_recv.at[s - 1], g, w).wait_recv()
        tot = jnp.sum(xr[j:j + NG], axis=0)
        for n in range(8):
            for c in range(3):
                fs[(s - 1) * 24 + 3 * n + c] = tot[n:n + 1, c * 128:(c + 1) * 128]
        for d in range(2):
            for dy in (2, 1, 3, 0):
                n = d * NY + dy
                f0 = (s - 1) * 24 + 3 * n
                if s == 8 and d == 1 and dy == 0:
                    for c in range(3):
                        lad[3 * w + c] = fs[f0 + c]
                else:
                    rcopy(
                        fs.at[pl.ds(f0, 3)], lad.at[pl.ds(3 * w, 3)], l_send, l_recv, g, wid(y + dy, col(s, d))
                    ).start()

    for i in range(1, 9):
        z_b(i + 1)
        if i > 1:
            comp_a(i - 1)
        if i == 1:
            y_b(0)
        y_b(i)
        z_a(i, 0)
        if i > 1:
            comp_b(i - 1, 0)
        z_a(i, 3)
        if i > 1:
            comp_b(i - 1, 1)
        z_a(i, 1)
        if i > 2:
            reduce(i - 2)
        z_a(i, 2)
    comp_a(8)
    comp_b(8, 0)
    comp_b(8, 1)
    reduce(7)
    reduce(8)

    part = pl.ds(0, 3 * (NW - 1))
    rcopy(fs.at[part], lad.at[part], l_send, l_recv, g, w).wait_recv()
    out[...] = (lad[...] + base3[...]) * inv3[...]

    rcopy(st0.at[pl.ds(0, 7)], st0.at[pl.ds(0, 7)], s0_send, s0_recv, g, w).wait_send()
    rcopy(stz, stz, sz_send, s0_recv, g, w).wait_send()
    rcopy(sty, sty, sy_send, s0_recv, g, w).wait_send()
    rcopy(ta.at[pl.ds(0, 60)], ta.at[pl.ds(0, 60)], ta_send, s0_recv, g, w).wait_send()
    rcopy(tb.at[pl.ds(0, 61)], tb.at[pl.ds(0, 61)], tb_send, s0_recv, g, w).wait_send()
    rcopy(sbuf.at[pl.ds(0, 56)], xr.at[pl.ds(0, 56)], x_send, x_recv.at[0], g, w).wait_send()
    rcopy(fs.at[part], lad.at[part], l_send, l_recv, g, w).wait_send()


def local(t, e, v, flags, f, r, hls, pls):
    any_spec = pl.BlockSpec(memory_space=pl.ANY)
    vm = pltpu.VMEM
    dma = pltpu.SemaphoreType.DMA
    res = pl.pallas_call(
        kernel,
        out_shape=jax.ShapeDtypeStruct((NQ, 1, 128), F32),
        in_specs=[any_spec] * 6 + [pl.BlockSpec(memory_space=pltpu.SMEM), any_spec],
        out_specs=pl.BlockSpec(memory_space=pltpu.VMEM),
        scratch_shapes=[
            vm((1, 24576), BF16),
            vm((1, 24576), BF16),
            vm((KG, Q), BF16),
            vm((6, 48), jnp.int32),
            vm((48, Q), F32),
            vm((6, 64, 64), F32),
            vm((6, 64, 64), F32),
            vm((NQ, 1, 128), F32),
            vm((NQ, 128), F32),
            vm((NQ, 128), F32),
            vm((NQ, 1, 128), F32),
            vm((NQ, 1, 128), F32),
            vm((NG, 24, 128), BF16),
            vm((NG, 24, 128), BF16),
            vm((2, NG, 16, 128), BF16),
            vm((3, NG, 8, 128), BF16),
            vm((NQ, 128), F32),
            vm((NW, 16, KA), BF16),
            vm((NW, 16, KB), BF16),
            vm((64, Q), F32),
            vm((3, 64, 128), F32),
            vm((64, 8, Q), F32),
            vm((64, 8, Q), F32),
            vm((NQ, 1, 128), F32),
            vm((NQ, 1, 128), F32),
            dma((7,)),
            dma,
            dma((2,)),
            dma((3,)),
            dma((2, 9, 4)),
            dma((2, 9)),
            dma((9, 2, 3)),
            dma((8,)),
            dma,
            dma,
            dma,
            dma,
            dma,
            dma,
            dma,
            dma,
        ],
        compiler_params=pltpu.CompilerParams(
            collective_id=0, has_side_effects=True, vmem_limit_bytes=60 * 1024 * 1024
        ),
        name="ladder",
    )(t, e, v, flags.T, f, r, hls, pls.reshape(NQ, 1, 128))
    return res.reshape(1, 24576)


def solution(mesh):
    return jax.shard_map(
        local,
        mesh=mesh,
        in_specs=(
            P(("grp", "wide"), None),
            P(("grp", "wide"), None),
            P("grp", "wide"),
            P("grp", "wide"),
            P(),
            P(),
            P(("grp", "wide")),
            P(),
        ),
        out_specs=P(("grp", "wide"), None),
        check_vma=False,
    )
```
